32 devices in a mesh: gx: 2 (over x), gy: 4 (over y, core), gz: 4 (over z).
Axes of the slice: x: 2, y: 2, z: 4, core: 2. Of those that a mesh axis runs over, the one named last changes fastest.
Arguments:
- right_side: float32 [24, 64, 512], P('gx', 'gy', 'gz'), may hold values from -8 to 8
- coefficient: float32 [24, 64, 512], P('gx', 'gy', 'gz'), may hold values from 0.02 to 1
Outputs:
- solution: float32 [24, 64, 512], P('gx', 'gy', 'gz')
- residual: float32 [24, 64, 512], P('gx', 'gy', 'gz')
- precond: float32 [24, 64, 512], P('gx', 'gy', 'gz')
- image: float32 [24, 64, 512], P('gx', 'gy', 'gz')
The draws below stay inside these ranges and needn't reach their ends.
All inputs are finite; a program needn't handle non-finite values.
Results may differ from the reference program's by a relative error of at most 0.00021.
Values sent between devices are 32-bit elements; how exact they have to be, the bound alone decides.
A program may use at most 64 MiB of HBM per device.

```python
import math
import jax
import jax.numpy as jnp

SWEEPS = 4
ITERS = 1
NX = 24
NY = 64
NZ = 512


def block_levels(own_key, shape, shards, smallest, largest):
    loudness, own = 1.0, jax.random.fold_in(own_key, 6)
    for position, parts in shards:
        steps = jnp.exp(jax.random.uniform(jax.random.fold_in(own, position), (parts,), jnp.float32, smallest / len(shards), largest / len(shards)))
        loudness = loudness * jnp.repeat(steps, shape[position] // parts).reshape([-1 if axis == position else 1 for axis in range(len(shape))])
    return loudness


def noise(own_key, shape, scale, reach, pieces=(), kind=jnp.bfloat16):
    values = jax.random.normal(own_key, shape, jnp.float32) * scale
    if len(pieces) > 0:
        values = block_levels(own_key, shape, pieces, -0.22, 0.18) * values
    return jnp.clip(values, min=-reach, max=reach).astype(kind)


def setup_inputs(seed: int = 0) -> dict:
    arg_keys = jax.random.split(jax.random.key(seed), 3)
    return {
        "right_side": noise(arg_keys[0], (NX, NY, NZ), 1.0, 8.0, ((0, 2), (1, 4), (2, 4)), jnp.float32),
        "coefficient": jnp.clip(jnp.exp(math.log(1.0) - 3.912023 * jax.random.uniform(arg_keys[1], (NX, NY, NZ), jnp.float32) ** block_levels(arg_keys[1], (NX, NY, NZ), ((0, 2), (1, 4), (2, 4)), -0.2, 0.2)), 0.02, 1.0),
    }


relaxation = 0.6


def block_sum(padded):
    summed = padded[:-2] + padded[1:-1] + padded[2:]
    summed = summed[:, :-2] + summed[:, 1:-1] + summed[:, 2:]
    return summed[:, :, :-2] + summed[:, :, 1:-1] + summed[:, :, 2:]


def operate(values, reaction):
    return (27.0 + reaction) * values - block_sum(jnp.pad(values, 1))


def restrict(values):
    extent = values.shape
    grouped = values.reshape(extent[0] // 2, 2, extent[1] // 2, 2, extent[2] // 2, 2)
    return 0.5 * grouped.sum(axis=(1, 3, 5))


def prolong(values):
    return jnp.repeat(jnp.repeat(jnp.repeat(values, 2, axis=0), 2, axis=1), 2, axis=2)


def coarsest(source, reaction):
    correction = relaxation * source / (26.0 + reaction)
    for sweep in range(SWEEPS - 1):
        correction = correction + relaxation * (source - operate(correction, reaction)) / (26.0 + reaction)
    return correction


def multigrid(source, reactions, level_index):
    if level_index == 2:
        return coarsest(source, reactions[2])
    reaction = reactions[level_index]
    correction = relaxation * source / (26.0 + reaction)
    remainder = source - operate(correction, reaction)
    correction = correction + prolong(multigrid(restrict(remainder), reactions, level_index + 1))
    return correction + relaxation * (source - operate(correction, reaction)) / (26.0 + reaction)


def reference(right_side, coefficient):
    middle = restrict(coefficient)
    reactions = (coefficient, middle, restrict(middle))
    solution = jnp.zeros_like(right_side)
    residual = right_side
    precond = multigrid(residual, reactions, 0)
    image = operate(precond, coefficient)
    direction = precond
    dir_image = image
    dir_precond = precond
    dir_twice = image
    gamma_prev = jnp.float32(1.0)
    alpha_prev = jnp.float32(1.0)
    for step in range(ITERS):
        gamma_now = jnp.sum(residual * precond)
        delta_now = jnp.sum(image * precond)
        precond_image = multigrid(image, reactions, 0)
        image_twice = operate(precond_image, coefficient)
        if step == 0:
            alpha_now = gamma_now / delta_now
            direction = precond
            dir_image = image
            dir_precond = precond_image
            dir_twice = image_twice
        else:
            beta_now = gamma_now / gamma_prev
            alpha_now = gamma_now / (delta_now - beta_now * gamma_now / alpha_prev)
            dir_twice = image_twice + beta_now * dir_twice
            dir_precond = precond_image + beta_now * dir_precond
            dir_image = image + beta_now * dir_image
            direction = precond + beta_now * direction
        solution = solution + alpha_now * direction
        residual = residual - alpha_now * dir_image
        precond = precond - alpha_now * dir_precond
        image = image - alpha_now * dir_twice
        gamma_prev = gamma_now
        alpha_prev = alpha_now
    return (solution, residual, precond, image)
```

```python
import functools

import jax
import jax.numpy as jnp
from jax import lax
from jax.experimental import pallas as pl
from jax.experimental.pallas import tpu as pltpu
from jax.sharding import PartitionSpec as P

SWEEPS = 4
relaxation = 0.6

AXES = ("gx", "gy", "gz")
MESH = pl.DeviceIdType.MESH
WIDTH = 5
EDGE = 8
SPAN = 2 * WIDTH
PART = SWEEPS


def dot(a, b):
    return jnp.dot(a, b, preferred_element_type=jnp.float32, precision=lax.Precision.HIGHEST)


def iota(shape, dim):
    return lax.broadcasted_iota(jnp.int32, shape, dim)


def kernel(counts, block, reach, g_ref, c_ref, sol_ref, res_ref, pre_ref, img_ref,
           gc0, im0, pk1, pk2, zr1, zr2, t1, d0, d1, xr0, xr1, pf0, pf1, xm, um,
           cs1, cs2, cr1, cr2, mid, red_s, red_r, ssem, rsem, lssem, lrsem):
    bx, by, bz = block
    kx = reach
    me = [lax.axis_index(a) for a in AXES]
    ex, ey = bx + SPAN, by + 2 * EDGE
    mx, my = bx // 2 + 4, ey // 2
    qx = bx // 4
    lane = iota((ey, bz), 1)
    row = iota((ey, bz), 0)

    def valid(offset):
        ok = None
        for axis, step in enumerate(offset):
            if step == 0:
                continue
            place = me[axis] + step
            term = place >= 0 if step < 0 else place < counts[axis]
            ok = term if ok is None else jnp.logical_and(ok, term)
        return ok

    def target(offset):
        return tuple(m + s for m, s in zip(me, offset))

    near = [(dx, dy, dz) for dx in range(-kx, kx + 1) for dy in (-1, 0, 1) for dz in (-1, 0, 1)]
    near = [o for o in near if o != (0, 0, 0) and all(counts[a] > abs(o[a]) for a in range(3))]
    close = [o for o in near if abs(o[0]) <= 1]

    barrier = pltpu.get_barrier_semaphore()
    lines = []
    for axis in range(3):
        for step in range(1, counts[axis]):
            to = list(me)
            to[axis] = lax.rem(me[axis] + step, counts[axis])
            lines.append((axis, step, tuple(to)))

    zr1[...] = jnp.zeros_like(zr1)
    zr2[...] = jnp.zeros_like(zr2)
    gc0[...] = jnp.zeros_like(gc0)
    im0[...] = jnp.zeros_like(im0)
    cr1[...] = jnp.zeros_like(cr1)
    cr2[...] = jnp.zeros_like(cr2)

    for offset in near:
        @pl.when(valid(offset))
        def _(offset=offset):
            pl.semaphore_signal(barrier, inc=1, device_id=target(offset), device_id_type=MESH)
    for axis, step, to in lines:
        pl.semaphore_signal(barrier, inc=1, device_id=to, device_id_type=MESH)

    def options(axis, far):
        total = 1
        for step in range(1, far + 1):
            if counts[axis] > step:
                total = total + (me[axis] >= step).astype(jnp.int32)
                total = total + (me[axis] + step < counts[axis]).astype(jnp.int32)
        return total

    greeted = options(0, kx) * options(1, 1) * options(2, 1) - 1 + len(lines)

    strip = (lane[:by] < WIDTH) | (lane[:by] >= bz - WIDTH)

    def packed(planes):
        total = None
        for i, plane in enumerate(planes):
            piece = jnp.where(strip, plane, 0.0)
            if i > 0:
                piece = pltpu.roll(piece, SPAN * i, 1)
            total = piece if total is None else total + piece
        return total

    def fill(buf, pk, s, planes):
        for i, plane in enumerate(planes):
            buf[s, WIDTH + i, EDGE:EDGE + by, :] = plane
        pk[s] = packed(planes)

    def row_ends(dy):
        if dy == 0:
            return 0, by, EDGE
        if dy > 0:
            return by - EDGE, EDGE, 0
        return 0, EDGE, EDGE + by

    def fine_copy(phase, n, offset, buf, pk, zr):
        dx, dy, dz = offset
        start, size, goes = row_ends(dy)
        if dz == 0:
            if dx == 0:
                px, nx, tx = WIDTH, bx, WIDTH
            elif dx > 0:
                px, nx, tx = bx, WIDTH, 0
            else:
                px, nx, tx = WIDTH, WIDTH, WIDTH + bx
            src = buf.at[:, pl.ds(px, nx), pl.ds(EDGE + start, size), :]
            dst = buf.at[:, pl.ds(tx, nx), pl.ds(goes, size), :]
        else:
            side = 0 if dz > 0 else 1
            src = pk.at[:, pl.ds(start, size), :]
            dst = zr.at[side, 1 - dx, :, pl.ds(goes, size), :]
        return pltpu.make_async_remote_copy(
            src_ref=src, dst_ref=dst, send_sem=ssem.at[phase, n], recv_sem=rsem.at[phase, n],
            device_id=target(offset), device_id_type=MESH)

    def coarse_copy(phase, n, offset, cs, cr):
        dx, dy, dz = offset
        return pltpu.make_async_remote_copy(
            src_ref=cs, dst_ref=cr.at[kx - dx, 1 - dy, 1 - dz],
            send_sem=ssem.at[phase, n], recv_sem=rsem.at[phase, n],
            device_id=target(offset), device_id_type=MESH)

    def begin(make, offsets):
        for n, offset in enumerate(offsets):
            @pl.when(valid(offset))
            def _(n=n, offset=offset):
                make(n, offset).start()

    def arrive(make, offsets):
        for n, offset in enumerate(offsets):
            @pl.when(valid(tuple(-s for s in offset)))
            def _(n=n, offset=offset):
                make(n, offset).wait_recv()

    def leave(make, offsets):
        for n, offset in enumerate(offsets):
            @pl.when(valid(offset))
            def _(n=n, offset=offset):
                make(n, offset).wait_send()

    def line_copy(axis, step, to):
        n = sum(counts[:axis]) + step
        return pltpu.make_async_remote_copy(
            src_ref=red_s.at[axis], dst_ref=red_r.at[n], send_sem=lssem.at[n],
            recv_sem=lrsem.at[n], device_id=to, device_id_type=MESH)

    def line_begin(axis, value):
        red_s[axis] = value
        for a, step, to in lines:
            if a == axis:
                line_copy(a, step, to).start()

    def line_end(axis):
        value = red_s[axis]
        for a, step, to in lines:
            if a == axis:
                line_copy(a, step, to).wait_recv()
                value = value + red_r[sum(counts[:a]) + step]
        return value

    place = lax.rem(lane + WIDTH, bz)
    low = lax.rem(place, SPAN) < WIDTH
    band = (lane < WIDTH) | (lane >= bz - WIDTH)

    def spread(zr, s, t):
        for side in range(3):
            merged = jnp.where(low, zr[0, side, s], zr[1, side, s])
            if side == 0:
                todo = [(bx - WIDTH + i, i) for i in range(WIDTH)]
            elif side == 1:
                todo = [(i, WIDTH + i) for i in range(bx)]
            else:
                todo = [(i, WIDTH + bx + i) for i in range(WIDTH)]
            for i, e in todo:
                piece = merged if i == 0 else pltpu.roll(merged, (bz - SPAN * i) % bz, 1)
                t1[t, e] = jnp.where(band, piece, 0.0)

    first, last = lane == 0, lane == bz - 1

    def yz(a, b):
        sa = a + jnp.where(first, pltpu.roll(b, 1, 1), pltpu.roll(a, 1, 1))
        sb = b + jnp.where(first, pltpu.roll(a, 1, 1), pltpu.roll(b, 1, 1))
        sa = sa + jnp.where(last, pltpu.roll(b, bz - 1, 1), pltpu.roll(a, bz - 1, 1))
        sb = sb + jnp.where(last, pltpu.roll(a, bz - 1, 1), pltpu.roll(b, bz - 1, 1))
        sa = sa + pltpu.roll(sa, 1, 0) + pltpu.roll(sa, ey - 1, 0)
        sb = sb + pltpu.roll(sb, 1, 0) + pltpu.roll(sb, ey - 1, 0)
        return sa, sb

    def box(v):
        s = v + pltpu.roll(v, 1, 2) + pltpu.roll(v, v.shape[2] - 1, 2)
        s = s + pltpu.roll(s, 1, 1) + pltpu.roll(s, v.shape[1] - 1, 1)
        zero = jnp.zeros_like(s[:1])
        return s + jnp.concatenate([zero, s[:-1]], 0) + jnp.concatenate([s[1:], zero], 0)

    p_, q_ = iota((bz, bz), 0), iota((bz, bz), 1)
    down_a = jnp.where((p_ >> 1) == q_, 0.5, 0.0)
    down_b = jnp.where(((p_ + bz) >> 1) == q_, 0.5, 0.0)
    up_a = jnp.where((q_ >> 1) == p_, 1.0, 0.0)
    up_b = jnp.where(((q_ + bz) >> 1) == p_, 1.0, 0.0)
    quarter = bz // 4
    down_c = jnp.where((p_ < bz // 2) & ((p_ >> 1) == lax.rem(q_, quarter)), 0.5, 0.0)
    up_c = jnp.where(p_ == jnp.where(q_ < 3 * quarter, q_ >> 1, (q_ >> 1) + bz // 2), 1.0, 0.0)

    def restricted(of):
        for m in range(mx):
            a0, b0 = of(2 * m + 1)
            a1, b1 = of(2 * m + 2)
            xr0[m * ey:(m + 1) * ey, :] = a0 + a1
            xr1[m * ey:(m + 1) * ey, :] = b0 + b1
        n = mx * my
        a = xr0[pl.ds(0, n, stride=2), :] + xr0[pl.ds(1, n, stride=2), :]
        b = xr1[pl.ds(0, n, stride=2), :] + xr1[pl.ds(1, n, stride=2), :]
        return (dot(a, down_a) + dot(b, down_b)).reshape(mx, my, bz)

    def coarsened(v):
        for m in range(qx):
            xm[m * my:(m + 1) * my, :] = v[2 + 2 * m] + v[3 + 2 * m]
        n = qx * my // 2
        a = xm[pl.ds(0, n, stride=2), :] + xm[pl.ds(1, n, stride=2), :]
        a = dot(a, down_c).reshape(qx, my // 2, bz)
        upper = iota(a.shape, 1) < my // 4
        return jnp.where(upper, pltpu.roll(a, my // 2 - 2, 1), pltpu.roll(a, 2, 1))

    clane = iota((my // 2, bz), 1)
    crow = iota((my // 2, bz), 0)
    xs = [x for x in range(-PART, qx + PART) if -kx * qx <= x < (kx + 1) * qx]

    def gathered(cr, cs, s):
        def tile(dx, dy, x):
            def piece(dz):
                if (dx, dy, dz) == (0, 0, 0):
                    return cs[s, x]
                return cr[kx + dx, 1 + dy, 1 + dz, s, x]
            v = jnp.where(clane >= 3 * quarter, piece(-1), piece(0))
            return jnp.where((clane >= quarter) & (clane < 2 * quarter), piece(1), v)

        planes = []
        for x in xs:
            dx = x // qx
            i = x - dx * qx
            upper = jnp.where(crow < my // 4, tile(dx, -1, i), tile(dx, 0, i))
            lower = jnp.where(crow < my // 4, tile(dx, 1, i), 0.0)
            planes.append(jnp.concatenate([upper, lower], 0))
        return jnp.stack(planes)

    def within(place, axis, size):
        place = place + me[axis] * size
        return (place >= 0) & (place < counts[axis] * size)

    g = [g_ref[i] for i in range(bx)]
    fill(gc0, pk1, 0, g)
    fill(gc0, pk1, 1, [c_ref[i] for i in range(bx)])
    pl.semaphore_wait(barrier, greeted)
    make_a = lambda n, o: fine_copy(0, n, o, gc0, pk1, zr1)
    begin(make_a, close)
    arrive(make_a, close)
    spread(zr1, 0, 0)
    spread(zr1, 1, 1)

    in_y = within(row - EDGE, 1, by)
    in_z = band & within(jnp.where(lane < bz // 2, lane + bz, lane - bz), 2, bz)
    for i in range(ex):
        in_x = within(jnp.full((ey, bz), i - WIDTH, jnp.int32), 0, bx)
        d0[i] = jnp.where(in_y & in_x, relaxation / (26.0 + gc0[1, i]), 0.0)
        d1[i] = jnp.where(in_y & in_x & in_z, relaxation / (26.0 + t1[1, i]), 0.0)

    c1 = restricted(lambda i: (gc0[1, i], t1[1, i]))
    shape = (mx, my, bz)
    zl = iota(shape, 2)
    zl = jnp.where(zl < 3 * quarter, zl, zl - bz)
    inside = within(iota(shape, 0) - 2, 0, bx // 2) & within(iota(shape, 1) - 4, 1, by // 2)
    inside = inside & within(zl, 2, bz // 2)
    mid[0] = jnp.where(inside, relaxation / (26.0 + c1), 0.0)
    mid[1] = 27.0 + c1
    cs1[1] = coarsened(c1)

    def inverse2(c2):
        shape = c2.shape
        z = iota(shape, 2)
        z = jnp.where(z < 2 * quarter, z, z - bz)
        ok = within(iota(shape, 0) + xs[0], 0, qx) & within(iota(shape, 1) - 4, 1, by // 4)
        ok = ok & within(z, 2, quarter) & (z >= -quarter)
        return jnp.where(ok, relaxation / (26.0 + c2), 0.0)

    def cycle(g_at, make_b, cs, cr, hook, second, finish):
        def e0(i):
            a, b = g_at(i)
            return d0[i] * a, d1[i] * b

        sums = {}

        def remainder(i):
            for k in (i - 1, i, i + 1):
                if k not in sums:
                    sums[k] = yz(*e0(k))
            a, b = g_at(i)
            ea, eb = e0(i)
            ra = a - (27.0 + gc0[1, i]) * ea + sums[i - 1][0] + sums[i][0] + sums[i + 1][0]
            rb = b - (27.0 + t1[1, i]) * eb + sums[i - 1][1] + sums[i][1] + sums[i + 1][1]
            return ra, rb

        g1 = restricted(remainder)
        f = mid[0] * g1
        mid[2] = g1
        cs[0] = coarsened(g1 - mid[1] * f + box(f))
        begin(make_b, near)
        hook()
        arrive(make_b, near)
        g2 = gathered(cr, cs, 0)
        c2 = gathered(cr1, cs1, 1)
        inv = inverse2(c2)
        diag = 27.0 + c2
        e = inv * g2
        for sweep in range(SWEEPS - 1):
            e = e + inv * (g2 - diag * e + box(e))
        second()
        nq = qx + 2
        e = jnp.concatenate([e[xs.index(x)][None] if x in xs else jnp.zeros_like(e[:1])
                             for x in range(-1, qx + 1)], 0)
        e = pltpu.roll(e, my - 2, 1)[:, :my // 2].reshape(nq * my // 2, bz)
        u = dot(e, up_c)
        um[pl.ds(0, nq * my // 2, stride=2), :] = u
        um[pl.ds(1, nq * my // 2, stride=2), :] = u
        u = um[...].reshape(nq, my, bz)
        u = jnp.concatenate([u[(m - 2) // 2 + 1][None] for m in range(mx)], 0)
        g1 = mid[2]
        f = mid[0] * g1 + u
        f = f + mid[0] * (g1 - mid[1] * f + box(f))
        nm = mx - 2
        f = f[1:mx - 1].reshape(nm * my, bz)
        for pf, up in ((pf0, up_a), (pf1, up_b)):
            w = dot(f, up)
            pf[pl.ds(0, nm * my, stride=2), :] = w
            pf[pl.ds(1, nm * my, stride=2), :] = w

        def e1(i):
            m = (i - WIDTH) // 2 + 1
            a, b = e0(i)
            return a + pf0[m * ey:(m + 1) * ey, :], b + pf1[m * ey:(m + 1) * ey, :]

        sums1, sums2 = {}, {}
        e2 = {}
        for i in range(WIDTH - 1, WIDTH + bx + 1):
            for k in (i - 1, i, i + 1):
                if k not in sums1:
                    sums1[k] = yz(*e1(k))
            ga, gb = g_at(i)
            ea, eb = e1(i)
            s = [sums1[i - 1][t] + sums1[i][t] + sums1[i + 1][t] for t in range(2)]
            za = ea + d0[i] * (ga - (27.0 + gc0[1, i]) * ea + s[0])
            zb = eb + d1[i] * (gb - (27.0 + t1[1, i]) * eb + s[1])
            e2[i] = za[EDGE:EDGE + by]
            sums2[i] = yz(za, zb)[0][EDGE:EDGE + by]
            k = i - 1
            if k - 1 in sums2:
                out = (27.0 + c_ref[k - WIDTH]) * e2[k] - (sums2[k - 1] + sums2[k] + sums2[k + 1])
                finish(k - WIDTH, e2[k], out)

    gamma, delta = [], []
    images = []

    def finish1(i, e, out):
        pre_ref[i] = e
        images.append(out)
        gamma.append(g_ref[i] * e)
        delta.append(out * e)

    nothing = lambda: None
    make_b = lambda n, o: coarse_copy(1, n, o, cs1, cr1)
    cycle(lambda i: (gc0[0, i], t1[0, i]), make_b, cs1, cr1, nothing, nothing, finish1)

    for i in range(bx):
        img_ref[i] = images[i]
    fill(im0, pk2, 0, images)
    make_c = lambda n, o: fine_copy(2, n, o, im0, pk2, zr2)
    begin(make_c, close)
    gs = jnp.sum(sum(gamma[1:], gamma[0]), axis=0, keepdims=True)
    ds = jnp.sum(sum(delta[1:], delta[0]), axis=0, keepdims=True)
    line_begin(2, jnp.where(iota((8, bz), 0) == 0, gs, ds))
    arrive(make_c, close)
    spread(zr2, 0, 2)

    state = []

    def hook():
        line_begin(1, line_end(2))

    def second():
        line_begin(0, line_end(1))

    def finish2(i, e, out):
        if not state:
            total = line_end(0)
            total = jnp.sum(total, axis=1, keepdims=True)
            state.append(total[0:1] / total[1:2])
        alpha = state[0]
        p, im = pre_ref[i], img_ref[i]
        sol_ref[i] = alpha * p
        res_ref[i] = g_ref[i] - alpha * im
        pre_ref[i] = p - alpha * e
        img_ref[i] = im - alpha * out

    make_d = lambda n, o: coarse_copy(3, n, o, cs2, cr2)
    cycle(lambda i: (im0[0, i], t1[2, i]), make_d, cs2, cr2, hook, second, finish2)

    leave(make_a, close)
    leave(make_b, near)
    leave(make_c, close)
    leave(make_d, near)
    for axis, step, to in lines:
        line_copy(axis, step, to).wait_send()


def solution(mesh):
    counts = tuple(mesh.shape[a] for a in AXES)

    def shards(right_side, coefficient):
        bx, by, bz = block = right_side.shape
        assert SPAN * bx <= bz and by == 16 and bx % 4 == 0
        kx = max(1, min(-(-PART // (bx // 4)), counts[0] - 1))
        ex, ey = bx + SPAN, by + 2 * EDGE
        mx, my = bx // 2 + 4, ey // 2
        qx = bx // 4
        most = (2 * kx + 1) * 9
        f32 = jnp.float32
        out = jax.ShapeDtypeStruct(block, f32)
        vmem = pl.BlockSpec(memory_space=pltpu.VMEM)
        return tuple(pl.pallas_call(
            functools.partial(kernel, counts, block, kx),
            out_shape=[out] * 4,
            in_specs=[vmem] * 2,
            out_specs=[vmem] * 4,
            scratch_shapes=[
                pltpu.VMEM((2, ex, ey, bz), f32),
                pltpu.VMEM((1, ex, ey, bz), f32),
                pltpu.VMEM((2, by, bz), f32),
                pltpu.VMEM((1, by, bz), f32),
                pltpu.VMEM((2, 3, 2, ey, bz), f32),
                pltpu.VMEM((2, 3, 1, ey, bz), f32),
                pltpu.VMEM((3, ex, ey, bz), f32),
                pltpu.VMEM((ex, ey, bz), f32),
                pltpu.VMEM((ex, ey, bz), f32),
                pltpu.VMEM((mx * ey, bz), f32),
                pltpu.VMEM((mx * ey, bz), f32),
                pltpu.VMEM(((mx - 2) * ey, bz), f32),
                pltpu.VMEM(((mx - 2) * ey, bz), f32),
                pltpu.VMEM((qx * my, bz), f32),
                pltpu.VMEM(((qx + 2) * my, bz), f32),
                pltpu.VMEM((2, qx, my // 2, bz), f32),
                pltpu.VMEM((1, qx, my // 2, bz), f32),
                pltpu.VMEM((2 * kx + 1, 3, 3, 2, qx, my // 2, bz), f32),
                pltpu.VMEM((2 * kx + 1, 3, 3, 1, qx, my // 2, bz), f32),
                pltpu.VMEM((3, mx, my, bz), f32),
                pltpu.VMEM((3, 8, bz), f32),
                pltpu.VMEM((sum(counts), 8, bz), f32),
                pltpu.SemaphoreType.DMA((4, most)),
                pltpu.SemaphoreType.DMA((4, most)),
                pltpu.SemaphoreType.DMA((sum(counts),)),
                pltpu.SemaphoreType.DMA((sum(counts),)),
            ],
            compiler_params=pltpu.CompilerParams(collective_id=0, has_side_effects=True),
            name="relayed",
        )(right_side, coefficient))

    placed = (P(*AXES), P(*AXES))
    return jax.shard_map(
        shards, mesh=mesh, in_specs=placed, out_specs=(P(*AXES),) * 4, check_vma=False
    )
```

```python
import functools

import jax
import jax.numpy as jnp
from jax import lax
from jax.experimental import pallas as pl
from jax.experimental.pallas import tpu as pltpu
from jax.sharding import PartitionSpec as P

SWEEPS = 4
relaxation = 0.6

AXES = ("gx", "gy", "gz")
MESH = pl.DeviceIdType.MESH
WIDTH = 5
EDGE = 8
SPAN = 2 * WIDTH
PART = SWEEPS


def dot(a, b):
    high = a.astype(jnp.bfloat16)
    low = (a - high.astype(jnp.float32)).astype(jnp.bfloat16)
    both = jnp.concatenate([high, low], 1)
    b = b.astype(jnp.bfloat16)
    return jnp.dot(both, jnp.concatenate([b, b], 0), preferred_element_type=jnp.float32)


def iota(shape, dim):
    return lax.broadcasted_iota(jnp.int32, shape, dim)


def kernel(counts, block, reach, g_ref, c_ref, pre_ref, img_ref, twice_ref, image_twice_ref, alpha_ref,
           gc0, im0, pk1, pk2, zr1, zr2, t1, d0, d1, xr0, xr1, pf0, pf1, xm, um,
           cs1, cs2, cr1, cr2, kept, mid, red_s, red_r, ssem, rsem, lssem, lrsem):
    bx, by, bz = block
    kx = reach
    me = [lax.axis_index(a) for a in AXES]
    ex, ey = bx + SPAN, by + 2 * EDGE
    mx, my = bx // 2 + 4, ey // 2
    qx = bx // 4
    lane = iota((ey, bz), 1)
    row = iota((ey, bz), 0)

    def valid(offset):
        ok = None
        for axis, step in enumerate(offset):
            if step == 0:
                continue
            place = me[axis] + step
            term = place >= 0 if step < 0 else place < counts[axis]
            ok = term if ok is None else jnp.logical_and(ok, term)
        return ok

    def target(offset):
        return tuple(m + s for m, s in zip(me, offset))

    near = [(dx, dy, dz) for dx in range(-kx, kx + 1) for dy in (-1, 0, 1) for dz in (-1, 0, 1)]
    near = [o for o in near if o != (0, 0, 0) and all(counts[a] > abs(o[a]) for a in range(3))]
    near.sort(key=lambda o: (-abs(o[0]), abs(o[1]) + abs(o[2])))
    close = [o for o in near if abs(o[0]) <= 1]

    barrier = pltpu.get_barrier_semaphore()
    lines = []
    for axis in range(3):
        for step in range(1, counts[axis]):
            to = list(me)
            to[axis] = lax.rem(me[axis] + step, counts[axis])
            lines.append((axis, step, tuple(to)))

    zr1[...] = jnp.zeros_like(zr1)
    zr2[...] = jnp.zeros_like(zr2)
    gc0[...] = jnp.zeros_like(gc0)
    im0[...] = jnp.zeros_like(im0)
    cr1[...] = jnp.zeros_like(cr1)
    cr2[...] = jnp.zeros_like(cr2)

    for offset in near:
        @pl.when(valid(offset))
        def _(offset=offset):
            pl.semaphore_signal(barrier, inc=1, device_id=target(offset), device_id_type=MESH)
    for axis, step, to in lines:
        pl.semaphore_signal(barrier, inc=1, device_id=to, device_id_type=MESH)

    def options(axis, far):
        total = 1
        for step in range(1, far + 1):
            if counts[axis] > step:
                total = total + (me[axis] >= step).astype(jnp.int32)
                total = total + (me[axis] + step < counts[axis]).astype(jnp.int32)
        return total

    greeted = options(0, kx) * options(1, 1) * options(2, 1) - 1 + len(lines)

    strip = (lane[:by] < WIDTH) | (lane[:by] >= bz - WIDTH)

    def packed(planes):
        total = None
        for i, plane in enumerate(planes):
            piece = jnp.where(strip, plane, 0.0)
            if i > 0:
                piece = pltpu.roll(piece, SPAN * i, 1)
            total = piece if total is None else total + piece
        return total

    def fill(buf, pk, s, planes):
        for i, plane in enumerate(planes):
            buf[s, WIDTH + i, EDGE:EDGE + by, :] = plane
        pk[s] = packed(planes)

    def row_ends(dy):
        if dy == 0:
            return 0, by, EDGE
        if dy > 0:
            return by - EDGE, EDGE, 0
        return 0, EDGE, EDGE + by

    def fine_copy(phase, n, offset, buf, pk, zr):
        dx, dy, dz = offset
        start, size, goes = row_ends(dy)
        if dz == 0:
            if dx == 0:
                px, nx, tx = WIDTH, bx, WIDTH
            elif dx > 0:
                px, nx, tx = bx, WIDTH, 0
            else:
                px, nx, tx = WIDTH, WIDTH, WIDTH + bx
            src = buf.at[:, pl.ds(px, nx), pl.ds(EDGE + start, size), :]
            dst = buf.at[:, pl.ds(tx, nx), pl.ds(goes, size), :]
        else:
            side = 0 if dz > 0 else 1
            src = pk.at[:, pl.ds(start, size), :]
            dst = zr.at[side, 1 - dx, :, pl.ds(goes, size), :]
        return pltpu.make_async_remote_copy(
            src_ref=src, dst_ref=dst, send_sem=ssem.at[phase, n], recv_sem=rsem.at[phase, n],
            device_id=target(offset), device_id_type=MESH)

    def coarse_copy(phase, n, offset, cs, cr):
        dx, dy, dz = offset
        return pltpu.make_async_remote_copy(
            src_ref=cs, dst_ref=cr.at[kx - dx, 1 - dy, 1 - dz],
            send_sem=ssem.at[phase, n], recv_sem=rsem.at[phase, n],
            device_id=target(offset), device_id_type=MESH)

    def begin(make, offsets):
        for n, offset in enumerate(offsets):
            @pl.when(valid(offset))
            def _(n=n, offset=offset):
                make(n, offset).start()

    def arrive(make, offsets):
        for n, offset in enumerate(offsets):
            @pl.when(valid(tuple(-s for s in offset)))
            def _(n=n, offset=offset):
                make(n, offset).wait_recv()

    def leave(make, offsets):
        for n, offset in enumerate(offsets):
            @pl.when(valid(offset))
            def _(n=n, offset=offset):
                make(n, offset).wait_send()

    def line_copy(axis, step, to):
        n = sum(counts[:axis]) + step
        return pltpu.make_async_remote_copy(
            src_ref=red_s.at[axis], dst_ref=red_r.at[n], send_sem=lssem.at[n],
            recv_sem=lrsem.at[n], device_id=to, device_id_type=MESH)

    def line_begin(axis, value):
        red_s[axis] = value
        for a, step, to in lines:
            if a == axis:
                line_copy(a, step, to).start()

    def line_end(axis):
        value = red_s[axis]
        for a, step, to in lines:
            if a == axis:
                line_copy(a, step, to).wait_recv()
                value = value + red_r[sum(counts[:a]) + step]
        return value

    place = lax.rem(lane + WIDTH, bz)
    low = lax.rem(place, SPAN) < WIDTH
    band = (lane < WIDTH) | (lane >= bz - WIDTH)

    def spread(zr, s, t):
        for side in range(3):
            merged = jnp.where(low, zr[0, side, s], zr[1, side, s])
            if side == 0:
                todo = [(bx - WIDTH + i, i) for i in range(WIDTH)]
            elif side == 1:
                todo = [(i, WIDTH + i) for i in range(bx)]
            else:
                todo = [(i, WIDTH + bx + i) for i in range(WIDTH)]
            for i, e in todo:
                piece = merged if i == 0 else pltpu.roll(merged, (bz - SPAN * i) % bz, 1)
                t1[t, e] = jnp.where(band, piece, 0.0)

    first, last = lane == 0, lane == bz - 1

    def yz(a, b):
        sa = a + jnp.where(first, pltpu.roll(b, 1, 1), pltpu.roll(a, 1, 1))
        sb = b + jnp.where(first, pltpu.roll(a, 1, 1), pltpu.roll(b, 1, 1))
        sa = sa + jnp.where(last, pltpu.roll(b, bz - 1, 1), pltpu.roll(a, bz - 1, 1))
        sb = sb + jnp.where(last, pltpu.roll(a, bz - 1, 1), pltpu.roll(b, bz - 1, 1))
        sa = sa + pltpu.roll(sa, 1, 0) + pltpu.roll(sa, ey - 1, 0)
        sb = sb + pltpu.roll(sb, 1, 0) + pltpu.roll(sb, ey - 1, 0)
        return sa, sb

    def box(v):
        s = v + pltpu.roll(v, 1, 2) + pltpu.roll(v, v.shape[2] - 1, 2)
        s = s + pltpu.roll(s, 1, 1) + pltpu.roll(s, v.shape[1] - 1, 1)
        zero = jnp.zeros_like(s[:1])
        return s + jnp.concatenate([zero, s[:-1]], 0) + jnp.concatenate([s[1:], zero], 0)

    p_, q_ = iota((bz, bz), 0), iota((bz, bz), 1)
    down_a = jnp.where((p_ >> 1) == q_, 0.5, 0.0)
    down_b = jnp.where(((p_ + bz) >> 1) == q_, 0.5, 0.0)
    up_a = jnp.where((q_ >> 1) == p_, 1.0, 0.0)
    up_b = jnp.where(((q_ + bz) >> 1) == p_, 1.0, 0.0)
    quarter = bz // 4
    down_c = jnp.where((p_ < bz // 2) & ((p_ >> 1) == lax.rem(q_, quarter)), 0.5, 0.0)
    up_c = jnp.where(p_ == jnp.where(q_ < 3 * quarter, q_ >> 1, (q_ >> 1) + bz // 2), 1.0, 0.0)

    def restricted(of):
        for m in range(mx):
            a0, b0 = of(2 * m + 1)
            a1, b1 = of(2 * m + 2)
            xr0[m * ey:(m + 1) * ey, :] = a0 + a1
            xr1[m * ey:(m + 1) * ey, :] = b0 + b1
        n = mx * my
        a = xr0[pl.ds(0, n, stride=2), :] + xr0[pl.ds(1, n, stride=2), :]
        b = xr1[pl.ds(0, n, stride=2), :] + xr1[pl.ds(1, n, stride=2), :]
        return (dot(a, down_a) + dot(b, down_b)).reshape(mx, my, bz)

    turn = iota((my // 2, bz), 1) // quarter
    crow = iota((my // 2, bz), 0)

    def coarsened(v, lift):
        for m in range(qx):
            xm[m * my:(m + 1) * my, :] = v[2 + 2 * m] + v[3 + 2 * m]
        n = qx * my // 2
        a = xm[pl.ds(0, n, stride=2), :] + xm[pl.ds(1, n, stride=2), :]
        a = dot(a, down_c)
        rows = my // 2
        tile = a[:rows]
        for m in range(1, qx):
            tile = jnp.where(turn == m, a[m * rows:(m + 1) * rows], tile)
        return pltpu.roll(tile, 2 if lift else rows - 2, 0)

    xs = [x for x in range(-PART, qx + PART) if -kx * qx <= x < (kx + 1) * qx]

    def gathered(cr, cs, lifts):
        half = my // 4
        columns = {}
        for dx in sorted({x // qx for x in xs}):
            for dy in (-1, 0, 1):
                here = cs[...] if (dx, dy) == (0, 0) else cr[kx + dx, 1 + dy, 1]
                after = pltpu.roll(cr[kx + dx, 1 + dy, 2], quarter, 1)
                before = pltpu.roll(cr[kx + dx, 1 + dy, 0], 3 * quarter, 1)
                for m in range(qx):
                    tile = jnp.where(turn == (m + 1) % 4, after, here)
                    tile = jnp.where(turn == (m + 3) % 4, before, tile)
                    if m > 0:
                        tile = pltpu.roll(tile, bz - quarter * m, 1)
                    columns[dx * qx + m, dy] = tile
        arrays = []
        for lift in lifts:
            planes = []
            for x in xs:
                tiles = [columns[x, dy] for dy in (-1, 0, 1)]
                turned = [pltpu.roll(t, half, 0) for t in tiles]
                if lift:
                    tiles, turned = turned, tiles
                upper = jnp.where(crow < half, tiles[0], turned[1])
                lower = jnp.where(crow < half, tiles[2], 0.0)
                planes.append(jnp.concatenate([upper, lower], 0))
            arrays.append(jnp.stack(planes))
        return arrays

    def within(place, axis, size):
        place = place + me[axis] * size
        return (place >= 0) & (place < counts[axis] * size)

    g = [g_ref[i] for i in range(bx)]
    fill(gc0, pk1, 0, g)
    fill(gc0, pk1, 1, [c_ref[i] for i in range(bx)])
    pl.semaphore_wait(barrier, greeted)
    make_a = lambda n, o: fine_copy(0, n, o, gc0, pk1, zr1)
    begin(make_a, close)
    arrive(make_a, close)
    spread(zr1, 0, 0)
    spread(zr1, 1, 1)

    in_y = within(row - EDGE, 1, by)
    in_z = band & within(jnp.where(lane < bz // 2, lane + bz, lane - bz), 2, bz)
    for i in range(ex):
        in_x = within(jnp.full((ey, bz), i - WIDTH, jnp.int32), 0, bx)
        d0[i] = jnp.where(in_y & in_x, relaxation / (26.0 + gc0[1, i]), 0.0)
        d1[i] = jnp.where(in_y & in_x & in_z, relaxation / (26.0 + t1[1, i]), 0.0)

    c1 = restricted(lambda i: (gc0[1, i], t1[1, i]))
    shape = (mx, my, bz)
    zl = iota(shape, 2)
    zl = jnp.where(zl < 3 * quarter, zl, zl - bz)
    inside = within(iota(shape, 0) - 2, 0, bx // 2) & within(iota(shape, 1) - 4, 1, by // 2)
    inside = inside & within(zl, 2, bz // 2)
    mid[0] = jnp.where(inside, relaxation / (26.0 + c1), 0.0)
    mid[1] = 27.0 + c1
    cs1[...] = coarsened(c1, True)

    def inverse2(c2):
        shape = c2.shape
        z = iota(shape, 2)
        z = jnp.where(z < 2 * quarter, z, z - bz)
        ok = within(iota(shape, 0) + xs[0], 0, qx) & within(iota(shape, 1) - 4, 1, by // 4)
        ok = ok & within(z, 2, quarter) & (z >= -quarter)
        return jnp.where(ok, relaxation / (26.0 + c2), 0.0)

    def cycle(g_at, make_b, cs, cr, hook, second, finish):
        def e0(i):
            a, b = g_at(i)
            return d0[i] * a, d1[i] * b

        sums = {}

        def remainder(i):
            for k in (i - 1, i, i + 1):
                if k not in sums:
                    sums[k] = yz(*e0(k))
            a, b = g_at(i)
            ea, eb = e0(i)
            ra = a - (27.0 + gc0[1, i]) * ea + sums[i - 1][0] + sums[i][0] + sums[i + 1][0]
            rb = b - (27.0 + t1[1, i]) * eb + sums[i - 1][1] + sums[i][1] + sums[i + 1][1]
            return ra, rb

        g1 = restricted(remainder)
        f = mid[0] * g1
        mid[2] = g1
        tile = coarsened(g1 - mid[1] * f + box(f), False)
        cs[...] = jnp.where(crow < my // 4, tile, cs1[...])
        begin(make_b, near)
        hook()
        arrive(make_b, near)
        if cr is cr1:
            g2, c2 = gathered(cr, cs, (False, True))
            kept[0] = inverse2(c2)
            kept[1] = 27.0 + c2
        else:
            g2, = gathered(cr, cs, (False,))
        inv, diag = kept[0], kept[1]
        e = inv * g2
        for sweep in range(SWEEPS - 1):
            e = e + inv * (g2 - diag * e + box(e))
        second()
        nq = qx + 2
        e = jnp.concatenate([e[xs.index(x)][None] if x in xs else jnp.zeros_like(e[:1])
                             for x in range(-1, qx + 1)], 0)
        e = pltpu.roll(e, my - 2, 1)[:, :my // 2].reshape(nq * my // 2, bz)
        u = dot(e, up_c)
        um[pl.ds(0, nq * my // 2, stride=2), :] = u
        um[pl.ds(1, nq * my // 2, stride=2), :] = u
        u = um[...].reshape(nq, my, bz)
        u = jnp.concatenate([u[(m - 2) // 2 + 1][None] for m in range(mx)], 0)
        g1 = mid[2]
        f = mid[0] * g1 + u
        f = f + mid[0] * (g1 - mid[1] * f + box(f))
        nm = mx - 2
        f = f[1:mx - 1].reshape(nm * my, bz)
        for pf, up in ((pf0, up_a), (pf1, up_b)):
            w = dot(f, up)
            pf[pl.ds(0, nm * my, stride=2), :] = w
            pf[pl.ds(1, nm * my, stride=2), :] = w

        def e1(i):
            m = (i - WIDTH) // 2 + 1
            a, b = e0(i)
            return a + pf0[m * ey:(m + 1) * ey, :], b + pf1[m * ey:(m + 1) * ey, :]

        sums1, sums2 = {}, {}
        e2 = {}
        for i in range(WIDTH - 1, WIDTH + bx + 1):
            for k in (i - 1, i, i + 1):
                if k not in sums1:
                    sums1[k] = yz(*e1(k))
            ga, gb = g_at(i)
            ea, eb = e1(i)
            s = [sums1[i - 1][t] + sums1[i][t] + sums1[i + 1][t] for t in range(2)]
            za = ea + d0[i] * (ga - (27.0 + gc0[1, i]) * ea + s[0])
            zb = eb + d1[i] * (gb - (27.0 + t1[1, i]) * eb + s[1])
            e2[i] = za[EDGE:EDGE + by]
            sums2[i] = yz(za, zb)[0][EDGE:EDGE + by]
            k = i - 1
            if k - 1 in sums2:
                out = (27.0 + c_ref[k - WIDTH]) * e2[k] - (sums2[k - 1] + sums2[k] + sums2[k + 1])
                finish(k - WIDTH, e2[k], out)

    gamma, delta = [], []
    images = []

    def finish1(i, e, out):
        pre_ref[i] = e
        images.append(out)
        gamma.append(g_ref[i] * e)
        delta.append(out * e)

    nothing = lambda: None
    make_b = lambda n, o: coarse_copy(1, n, o, cs1, cr1)
    cycle(lambda i: (gc0[0, i], t1[0, i]), make_b, cs1, cr1, nothing, nothing, finish1)

    for i in range(bx):
        img_ref[i] = images[i]
    fill(im0, pk2, 0, images)
    make_c = lambda n, o: fine_copy(2, n, o, im0, pk2, zr2)
    begin(make_c, close)
    gs = jnp.sum(sum(gamma[1:], gamma[0]), axis=0, keepdims=True)
    ds = jnp.sum(sum(delta[1:], delta[0]), axis=0, keepdims=True)
    line_begin(2, jnp.where(iota((8, bz), 0) == 0, gs, ds))
    arrive(make_c, close)
    spread(zr2, 0, 2)

    def hook():
        line_begin(1, line_end(2))

    def second():
        line_begin(0, line_end(1))

    def finish2(i, e, out):
        twice_ref[i] = e
        image_twice_ref[i] = out

    make_d = lambda n, o: coarse_copy(3, n, o, cs2, cr2)
    cycle(lambda i: (im0[0, i], t1[2, i]), make_d, cs2, cr2, hook, second, finish2)

    total = jnp.sum(line_end(0), axis=1, keepdims=True)
    alpha_ref[...] = jnp.broadcast_to(total[0:1] / total[1:2], alpha_ref.shape)
    leave(make_a, close)
    leave(make_b, near)
    leave(make_c, close)
    leave(make_d, near)
    for axis, step, to in lines:
        line_copy(axis, step, to).wait_send()


def solution(mesh):
    counts = tuple(mesh.shape[a] for a in AXES)

    def shards(right_side, coefficient):
        bx, by, bz = block = right_side.shape
        assert SPAN * bx <= bz and by == 16 and bx % 4 == 0
        kx = max(1, min(-(-PART // (bx // 4)), counts[0] - 1))
        ex, ey = bx + SPAN, by + 2 * EDGE
        mx, my = bx // 2 + 4, ey // 2
        qx = bx // 4
        most = (2 * kx + 1) * 9
        planes = qx + 2 * min(PART, kx * qx)
        f32 = jnp.float32
        out = jax.ShapeDtypeStruct(block, f32)
        vmem = pl.BlockSpec(memory_space=pltpu.VMEM)
        precond, image, twice, image_twice, alpha = pl.pallas_call(
            functools.partial(kernel, counts, block, kx),
            out_shape=[out] * 4 + [jax.ShapeDtypeStruct((8, bz), f32)],
            in_specs=[vmem] * 2,
            out_specs=[vmem] * 5,
            scratch_shapes=[
                pltpu.VMEM((2, ex, ey, bz), f32),
                pltpu.VMEM((1, ex, ey, bz), f32),
                pltpu.VMEM((2, by, bz), f32),
                pltpu.VMEM((1, by, bz), f32),
                pltpu.VMEM((2, 3, 2, ey, bz), f32),
                pltpu.VMEM((2, 3, 1, ey, bz), f32),
                pltpu.VMEM((3, ex, ey, bz), f32),
                pltpu.VMEM((ex, ey, bz), f32),
                pltpu.VMEM((ex, ey, bz), f32),
                pltpu.VMEM((mx * ey, bz), f32),
                pltpu.VMEM((mx * ey, bz), f32),
                pltpu.VMEM(((mx - 2) * ey, bz), f32),
                pltpu.VMEM(((mx - 2) * ey, bz), f32),
                pltpu.VMEM((qx * my, bz), f32),
                pltpu.VMEM(((qx + 2) * my, bz), f32),
                pltpu.VMEM((my // 2, bz), f32),
                pltpu.VMEM((my // 2, bz), f32),
                pltpu.VMEM((2 * kx + 1, 3, 3, my // 2, bz), f32),
                pltpu.VMEM((2 * kx + 1, 3, 3, my // 2, bz), f32),
                pltpu.VMEM((2, planes, my, bz), f32),
                pltpu.VMEM((3, mx, my, bz), f32),
                pltpu.VMEM((3, 8, bz), f32),
                pltpu.VMEM((sum(counts), 8, bz), f32),
                pltpu.SemaphoreType.DMA((4, most)),
                pltpu.SemaphoreType.DMA((4, most)),
                pltpu.SemaphoreType.DMA((sum(counts),)),
                pltpu.SemaphoreType.DMA((sum(counts),)),
            ],
            compiler_params=pltpu.CompilerParams(collective_id=0, has_side_effects=True),
            name="relayed",
        )(right_side, coefficient)
        alpha = alpha[0]
        return (alpha * precond, right_side - alpha * image,
                precond - alpha * twice, image - alpha * image_twice)

    placed = (P(*AXES), P(*AXES))
    return jax.shard_map(
        shards, mesh=mesh, in_specs=placed, out_specs=(P(*AXES),) * 4, check_vma=False
    )
```

```python
import functools

import jax
import jax.numpy as jnp
from jax import lax
from jax.experimental import pallas as pl
from jax.experimental.pallas import tpu as pltpu
from jax.sharding import PartitionSpec as P

SWEEPS = 4
relaxation = 0.6

AXES = ("gx", "gy", "gz")
MESH = pl.DeviceIdType.MESH
WIDTH = 5
EDGE = 8
SPAN = 2 * WIDTH
PART = SWEEPS


def dot(a, b):
    high = a.astype(jnp.bfloat16)
    low = (a - high.astype(jnp.float32)).astype(jnp.bfloat16)
    both = jnp.concatenate([high, low], 1)
    b = b.astype(jnp.bfloat16)
    return jnp.dot(both, jnp.concatenate([b, b], 0), preferred_element_type=jnp.float32)


def iota(shape, dim):
    return lax.broadcasted_iota(jnp.int32, shape, dim)


def kernel(counts, block, reach, g_ref, c_ref, pre_ref, img_ref, twice_ref, image_twice_ref, alpha_ref,
           gc0, im0, pk1, pk2, zr1, zr2, t1, d0, d1, xr0, xr1, pf0, pf1, xm, um,
           cs1, cs2, cr1, cr2, kept, mid, red_s, red_r, ssem, rsem, lssem, lrsem):
    bx, by, bz = block
    kx = reach
    me = [lax.axis_index(a) for a in AXES]
    ex, ey = bx + SPAN, by + 2 * EDGE
    mx, my = bx // 2 + 4, ey // 2
    qx = bx // 4
    lane = iota((ey, bz), 1)
    row = iota((ey, bz), 0)

    def valid(offset):
        ok = None
        for axis, step in enumerate(offset):
            if step == 0:
                continue
            place = me[axis] + step
            term = place >= 0 if step < 0 else place < counts[axis]
            ok = term if ok is None else jnp.logical_and(ok, term)
        return ok

    def target(offset):
        return tuple(m + s for m, s in zip(me, offset))

    near = [(dx, dy, dz) for dx in range(-kx, kx + 1) for dy in (-1, 0, 1) for dz in (-1, 0, 1)]
    near = [o for o in near if o != (0, 0, 0) and all(counts[a] > abs(o[a]) for a in range(3))]
    near.sort(key=lambda o: (-abs(o[0]), abs(o[1]) + abs(o[2])))
    close = [o for o in near if abs(o[0]) <= 1]

    barrier = pltpu.get_barrier_semaphore()
    lines = []
    for axis in range(3):
        for step in range(1, counts[axis]):
            to = list(me)
            to[axis] = lax.rem(me[axis] + step, counts[axis])
            lines.append((axis, step, tuple(to)))

    zr1[...] = jnp.zeros_like(zr1)
    gc0[...] = jnp.zeros_like(gc0)
    cr1[...] = jnp.zeros_like(cr1)

    for offset in near:
        @pl.when(valid(offset))
        def _(offset=offset):
            pl.semaphore_signal(barrier, inc=1, device_id=target(offset), device_id_type=MESH)
    for axis, step, to in lines:
        pl.semaphore_signal(barrier, inc=1, device_id=to, device_id_type=MESH)

    def options(axis, far):
        total = 1
        for step in range(1, far + 1):
            if counts[axis] > step:
                total = total + (me[axis] >= step).astype(jnp.int32)
                total = total + (me[axis] + step < counts[axis]).astype(jnp.int32)
        return total

    greeted = options(0, kx) * options(1, 1) * options(2, 1) - 1 + len(lines)

    strip = (lane[:by] < WIDTH) | (lane[:by] >= bz - WIDTH)

    def packed(planes):
        total = None
        for i, plane in enumerate(planes):
            piece = jnp.where(strip, plane, 0.0)
            if i > 0:
                piece = pltpu.roll(piece, SPAN * i, 1)
            total = piece if total is None else total + piece
        return total

    def fill(buf, pk, s, planes):
        for i, plane in enumerate(planes):
            buf[s, WIDTH + i, EDGE:EDGE + by, :] = plane
        pk[s] = packed(planes)

    def row_ends(dy):
        if dy == 0:
            return 0, by, EDGE
        if dy > 0:
            return by - EDGE, EDGE, 0
        return 0, EDGE, EDGE + by

    def fine_copy(phase, n, offset, buf, pk, zr):
        dx, dy, dz = offset
        start, size, goes = row_ends(dy)
        if dz == 0:
            if dx == 0:
                px, nx, tx = WIDTH, bx, WIDTH
            elif dx > 0:
                px, nx, tx = bx, WIDTH, 0
            else:
                px, nx, tx = WIDTH, WIDTH, WIDTH + bx
            src = buf.at[:, pl.ds(px, nx), pl.ds(EDGE + start, size), :]
            dst = buf.at[:, pl.ds(tx, nx), pl.ds(goes, size), :]
        else:
            side = 0 if dz > 0 else 1
            src = pk.at[:, pl.ds(start, size), :]
            dst = zr.at[side, 1 - dx, :, pl.ds(goes, size), :]
        return pltpu.make_async_remote_copy(
            src_ref=src, dst_ref=dst, send_sem=ssem.at[phase, n], recv_sem=rsem.at[phase, n],
            device_id=target(offset), device_id_type=MESH)

    def coarse_copy(phase, n, offset, cs, cr):
        dx, dy, dz = offset
        return pltpu.make_async_remote_copy(
            src_ref=cs, dst_ref=cr.at[kx - dx, 1 - dy, 1 - dz],
            send_sem=ssem.at[phase, n], recv_sem=rsem.at[phase, n],
            device_id=target(offset), device_id_type=MESH)

    def begin(make, offsets):
        for n, offset in enumerate(offsets):
            @pl.when(valid(offset))
            def _(n=n, offset=offset):
                make(n, offset).start()

    def arrive(make, offsets):
        for n, offset in enumerate(offsets):
            @pl.when(valid(tuple(-s for s in offset)))
            def _(n=n, offset=offset):
                make(n, offset).wait_recv()

    def leave(make, offsets):
        for n, offset in enumerate(offsets):
            @pl.when(valid(offset))
            def _(n=n, offset=offset):
                make(n, offset).wait_send()

    def line_copy(axis, step, to):
        n = sum(counts[:axis]) + step
        return pltpu.make_async_remote_copy(
            src_ref=red_s.at[axis], dst_ref=red_r.at[n], send_sem=lssem.at[n],
            recv_sem=lrsem.at[n], device_id=to, device_id_type=MESH)

    def line_begin(axis, value):
        red_s[axis] = value
        for a, step, to in lines:
            if a == axis:
                line_copy(a, step, to).start()

    def line_end(axis):
        value = red_s[axis]
        for a, step, to in lines:
            if a == axis:
                line_copy(a, step, to).wait_recv()
                value = value + red_r[sum(counts[:a]) + step]
        return value

    place = lax.rem(lane + WIDTH, bz)
    low = lax.rem(place, SPAN) < WIDTH
    band = (lane < WIDTH) | (lane >= bz - WIDTH)

    def spread(zr, s, t):
        for side in range(3):
            merged = jnp.where(low, zr[0, side, s], zr[1, side, s])
            if side == 0:
                todo = [(bx - WIDTH + i, i) for i in range(WIDTH)]
            elif side == 1:
                todo = [(i, WIDTH + i) for i in range(bx)]
            else:
                todo = [(i, WIDTH + bx + i) for i in range(WIDTH)]
            for i, e in todo:
                piece = merged if i == 0 else pltpu.roll(merged, (bz - SPAN * i) % bz, 1)
                t1[t, e] = jnp.where(band, piece, 0.0)

    first, last = lane == 0, lane == bz - 1

    def yz(a, b):
        sa = a + jnp.where(first, pltpu.roll(b, 1, 1), pltpu.roll(a, 1, 1))
        sb = b + jnp.where(first, pltpu.roll(a, 1, 1), pltpu.roll(b, 1, 1))
        sa = sa + jnp.where(last, pltpu.roll(b, bz - 1, 1), pltpu.roll(a, bz - 1, 1))
        sb = sb + jnp.where(last, pltpu.roll(a, bz - 1, 1), pltpu.roll(b, bz - 1, 1))
        sa = sa + pltpu.roll(sa, 1, 0) + pltpu.roll(sa, ey - 1, 0)
        sb = sb + pltpu.roll(sb, 1, 0) + pltpu.roll(sb, ey - 1, 0)
        return sa, sb

    def box(v):
        s = v + pltpu.roll(v, 1, 2) + pltpu.roll(v, v.shape[2] - 1, 2)
        s = s + pltpu.roll(s, 1, 1) + pltpu.roll(s, v.shape[1] - 1, 1)
        zero = jnp.zeros_like(s[:1])
        return s + jnp.concatenate([zero, s[:-1]], 0) + jnp.concatenate([s[1:], zero], 0)

    p_, q_ = iota((bz, bz), 0), iota((bz, bz), 1)
    down_a = jnp.where((p_ >> 1) == q_, 0.5, 0.0)
    down_b = jnp.where(((p_ + bz) >> 1) == q_, 0.5, 0.0)
    up_a = jnp.where((q_ >> 1) == p_, 1.0, 0.0)
    up_b = jnp.where(((q_ + bz) >> 1) == p_, 1.0, 0.0)
    quarter = bz // 4
    down_c = jnp.where((p_ < bz // 2) & ((p_ >> 1) == lax.rem(q_, quarter)), 0.5, 0.0)
    up_c = jnp.where(p_ == jnp.where(q_ < 3 * quarter, q_ >> 1, (q_ >> 1) + bz // 2), 1.0, 0.0)

    def restricted(of):
        for m in range(mx):
            a0, b0 = of(2 * m + 1)
            a1, b1 = of(2 * m + 2)
            xr0[m * ey:(m + 1) * ey, :] = a0 + a1
            xr1[m * ey:(m + 1) * ey, :] = b0 + b1
        n = mx * my
        a = xr0[pl.ds(0, n, stride=2), :] + xr0[pl.ds(1, n, stride=2), :]
        b = xr1[pl.ds(0, n, stride=2), :] + xr1[pl.ds(1, n, stride=2), :]
        return (dot(a, down_a) + dot(b, down_b)).reshape(mx, my, bz)

    turn = iota((my // 2, bz), 1) // quarter
    crow = iota((my // 2, bz), 0)

    def coarsened(v, lift):
        for m in range(qx):
            xm[m * my:(m + 1) * my, :] = v[2 + 2 * m] + v[3 + 2 * m]
        n = qx * my // 2
        a = xm[pl.ds(0, n, stride=2), :] + xm[pl.ds(1, n, stride=2), :]
        a = dot(a, down_c)
        rows = my // 2
        tile = a[:rows]
        for m in range(1, qx):
            tile = jnp.where(turn == m, a[m * rows:(m + 1) * rows], tile)
        return pltpu.roll(tile, 2 if lift else rows - 2, 0)

    xs = [x for x in range(-PART, qx + PART) if -kx * qx <= x < (kx + 1) * qx]

    def gathered(cr, cs, lifts):
        half = my // 4
        columns = {}
        for dx in sorted({x // qx for x in xs}):
            for dy in (-1, 0, 1):
                here = cs[...] if (dx, dy) == (0, 0) else cr[kx + dx, 1 + dy, 1]
                after = pltpu.roll(cr[kx + dx, 1 + dy, 2], quarter, 1)
                before = pltpu.roll(cr[kx + dx, 1 + dy, 0], 3 * quarter, 1)
                for m in range(qx):
                    tile = jnp.where(turn == (m + 1) % 4, after, here)
                    tile = jnp.where(turn == (m + 3) % 4, before, tile)
                    if m > 0:
                        tile = pltpu.roll(tile, bz - quarter * m, 1)
                    columns[dx * qx + m, dy] = tile
        arrays = []
        for lift in lifts:
            planes = []
            for x in xs:
                tiles = [columns[x, dy] for dy in (-1, 0, 1)]
                turned = [pltpu.roll(t, half, 0) for t in tiles]
                if lift:
                    tiles, turned = turned, tiles
                upper = jnp.where(crow < half, tiles[0], turned[1])
                lower = jnp.where(crow < half, tiles[2], 0.0)
                planes.append(jnp.concatenate([upper, lower], 0))
            arrays.append(jnp.stack(planes))
        return arrays

    def within(place, axis, size):
        place = place + me[axis] * size
        return (place >= 0) & (place < counts[axis] * size)

    g = [g_ref[i] for i in range(bx)]
    fill(gc0, pk1, 0, g)
    fill(gc0, pk1, 1, [c_ref[i] for i in range(bx)])
    for buf in (zr2, im0, cr2):
        buf[...] = jnp.zeros_like(buf)
    pl.semaphore_wait(barrier, greeted)
    make_a = lambda n, o: fine_copy(0, n, o, gc0, pk1, zr1)
    begin(make_a, close)
    arrive(make_a, close)
    spread(zr1, 0, 0)
    spread(zr1, 1, 1)

    in_y = within(row - EDGE, 1, by)
    in_z = band & within(jnp.where(lane < bz // 2, lane + bz, lane - bz), 2, bz)
    for i in range(ex):
        in_x = within(jnp.full((ey, bz), i - WIDTH, jnp.int32), 0, bx)
        d0[i] = jnp.where(in_y & in_x, relaxation / (26.0 + gc0[1, i]), 0.0)
        d1[i] = jnp.where(in_y & in_x & in_z, relaxation / (26.0 + t1[1, i]), 0.0)

    c1 = restricted(lambda i: (gc0[1, i], t1[1, i]))
    shape = (mx, my, bz)
    zl = iota(shape, 2)
    zl = jnp.where(zl < 3 * quarter, zl, zl - bz)
    inside = within(iota(shape, 0) - 2, 0, bx // 2) & within(iota(shape, 1) - 4, 1, by // 2)
    inside = inside & within(zl, 2, bz // 2)
    mid[0] = jnp.where(inside, relaxation / (26.0 + c1), 0.0)
    mid[1] = 27.0 + c1
    cs1[...] = coarsened(c1, True)

    def inverse2(c2):
        shape = c2.shape
        z = iota(shape, 2)
        z = jnp.where(z < 2 * quarter, z, z - bz)
        ok = within(iota(shape, 0) + xs[0], 0, qx) & within(iota(shape, 1) - 4, 1, by // 4)
        ok = ok & within(z, 2, quarter) & (z >= -quarter)
        return jnp.where(ok, relaxation / (26.0 + c2), 0.0)

    def cycle(g_at, make_b, cs, cr, hook, second, finish):
        def e0(i):
            a, b = g_at(i)
            return d0[i] * a, d1[i] * b

        sums = {}

        def remainder(i):
            for k in (i - 1, i, i + 1):
                if k not in sums:
                    sums[k] = yz(*e0(k))
            a, b = g_at(i)
            ea, eb = e0(i)
            ra = a - (27.0 + gc0[1, i]) * ea + sums[i - 1][0] + sums[i][0] + sums[i + 1][0]
            rb = b - (27.0 + t1[1, i]) * eb + sums[i - 1][1] + sums[i][1] + sums[i + 1][1]
            return ra, rb

        g1 = restricted(remainder)
        f = mid[0] * g1
        mid[2] = g1
        tile = coarsened(g1 - mid[1] * f + box(f), False)
        cs[...] = jnp.where(crow < my // 4, tile, cs1[...])
        begin(make_b, near)
        hook()
        arrive(make_b, near)
        if cr is cr1:
            g2, c2 = gathered(cr, cs, (False, True))
            kept[0] = inverse2(c2)
            kept[1] = 27.0 + c2
        else:
            g2, = gathered(cr, cs, (False,))
        inv, diag = kept[0], kept[1]
        e = inv * g2
        for sweep in range(SWEEPS - 1):
            e = e + inv * (g2 - diag * e + box(e))
        second()
        nq = qx + 2
        e = jnp.concatenate([e[xs.index(x)][None] if x in xs else jnp.zeros_like(e[:1])
                             for x in range(-1, qx + 1)], 0)
        e = pltpu.roll(e, my - 2, 1)[:, :my // 2].reshape(nq * my // 2, bz)
        u = dot(e, up_c)
        um[pl.ds(0, nq * my // 2, stride=2), :] = u
        um[pl.ds(1, nq * my // 2, stride=2), :] = u
        u = um[...].reshape(nq, my, bz)
        u = jnp.concatenate([u[(m - 2) // 2 + 1][None] for m in range(mx)], 0)
        g1 = mid[2]
        f = mid[0] * g1 + u
        f = f + mid[0] * (g1 - mid[1] * f + box(f))
        nm = mx - 2
        f = f[1:mx - 1].reshape(nm * my, bz)
        for pf, up in ((pf0, up_a), (pf1, up_b)):
            w = dot(f, up)
            pf[pl.ds(0, nm * my, stride=2), :] = w
            pf[pl.ds(1, nm * my, stride=2), :] = w

        def e1(i):
            m = (i - WIDTH) // 2 + 1
            a, b = e0(i)
            return a + pf0[m * ey:(m + 1) * ey, :], b + pf1[m * ey:(m + 1) * ey, :]

        sums1, sums2 = {}, {}
        e2 = {}
        for i in range(WIDTH - 1, WIDTH + bx + 1):
            for k in (i - 1, i, i + 1):
                if k not in sums1:
                    sums1[k] = yz(*e1(k))
            ga, gb = g_at(i)
            ea, eb = e1(i)
            s = [sums1[i - 1][t] + sums1[i][t] + sums1[i + 1][t] for t in range(2)]
            za = ea + d0[i] * (ga - (27.0 + gc0[1, i]) * ea + s[0])
            zb = eb + d1[i] * (gb - (27.0 + t1[1, i]) * eb + s[1])
            e2[i] = za[EDGE:EDGE + by]
            sums2[i] = yz(za, zb)[0][EDGE:EDGE + by]
            k = i - 1
            if k - 1 in sums2:
                out = (27.0 + c_ref[k - WIDTH]) * e2[k] - (sums2[k - 1] + sums2[k] + sums2[k + 1])
                finish(k - WIDTH, e2[k], out)

    gamma, delta = [], []
    images = []

    def finish1(i, e, out):
        pre_ref[i] = e
        images.append(out)
        gamma.append(g_ref[i] * e)
        delta.append(out * e)

    nothing = lambda: None
    make_b = lambda n, o: coarse_copy(1, n, o, cs1, cr1)
    cycle(lambda i: (gc0[0, i], t1[0, i]), make_b, cs1, cr1, nothing, nothing, finish1)

    for i in range(bx):
        img_ref[i] = images[i]
    fill(im0, pk2, 0, images)
    make_c = lambda n, o: fine_copy(2, n, o, im0, pk2, zr2)
    begin(make_c, close)
    gs = jnp.sum(sum(gamma[1:], gamma[0]), axis=0, keepdims=True)
    ds = jnp.sum(sum(delta[1:], delta[0]), axis=0, keepdims=True)
    line_begin(2, jnp.where(iota((8, bz), 0) == 0, gs, ds))
    arrive(make_c, close)
    spread(zr2, 0, 2)

    def hook():
        line_begin(1, line_end(2))

    def second():
        line_begin(0, line_end(1))

    def finish2(i, e, out):
        twice_ref[i] = e
        image_twice_ref[i] = out

    make_d = lambda n, o: coarse_copy(3, n, o, cs2, cr2)
    cycle(lambda i: (im0[0, i], t1[2, i]), make_d, cs2, cr2, hook, second, finish2)

    total = jnp.sum(line_end(0), axis=1, keepdims=True)
    alpha_ref[...] = jnp.broadcast_to(total[0:1] / total[1:2], alpha_ref.shape)
    leave(make_a, close)
    leave(make_b, near)
    leave(make_c, close)
    leave(make_d, near)
    for axis, step, to in lines:
        line_copy(axis, step, to).wait_send()


def solution(mesh):
    counts = tuple(mesh.shape[a] for a in AXES)

    def shards(right_side, coefficient):
        bx, by, bz = block = right_side.shape
        assert SPAN * bx <= bz and by == 16 and bx % 4 == 0
        kx = max(1, min(-(-PART // (bx // 4)), counts[0] - 1))
        ex, ey = bx + SPAN, by + 2 * EDGE
        mx, my = bx // 2 + 4, ey // 2
        qx = bx // 4
        most = (2 * kx + 1) * 9
        planes = qx + 2 * min(PART, kx * qx)
        f32 = jnp.float32
        out = jax.ShapeDtypeStruct(block, f32)
        vmem = pl.BlockSpec(memory_space=pltpu.VMEM)
        precond, image, twice, image_twice, alpha = pl.pallas_call(
            functools.partial(kernel, counts, block, kx),
            out_shape=[out] * 4 + [jax.ShapeDtypeStruct((1, 1, bz), f32)],
            in_specs=[vmem] * 2,
            out_specs=[vmem] * 5,
            scratch_shapes=[
                pltpu.VMEM((2, ex, ey, bz), f32),
                pltpu.VMEM((1, ex, ey, bz), f32),
                pltpu.VMEM((2, by, bz), f32),
                pltpu.VMEM((1, by, bz), f32),
                pltpu.VMEM((2, 3, 2, ey, bz), f32),
                pltpu.VMEM((2, 3, 1, ey, bz), f32),
                pltpu.VMEM((3, ex, ey, bz), f32),
                pltpu.VMEM((ex, ey, bz), f32),
                pltpu.VMEM((ex, ey, bz), f32),
                pltpu.VMEM((mx * ey, bz), f32),
                pltpu.VMEM((mx * ey, bz), f32),
                pltpu.VMEM(((mx - 2) * ey, bz), f32),
                pltpu.VMEM(((mx - 2) * ey, bz), f32),
                pltpu.VMEM((qx * my, bz), f32),
                pltpu.VMEM(((qx + 2) * my, bz), f32),
                pltpu.VMEM((my // 2, bz), f32),
                pltpu.VMEM((my // 2, bz), f32),
                pltpu.VMEM((2 * kx + 1, 3, 3, my // 2, bz), f32),
                pltpu.VMEM((2 * kx + 1, 3, 3, my // 2, bz), f32),
                pltpu.VMEM((2, planes, my, bz), f32),
                pltpu.VMEM((3, mx, my, bz), f32),
                pltpu.VMEM((3, 8, bz), f32),
                pltpu.VMEM((sum(counts), 8, bz), f32),
                pltpu.SemaphoreType.DMA((4, most)),
                pltpu.SemaphoreType.DMA((4, most)),
                pltpu.SemaphoreType.DMA((sum(counts),)),
                pltpu.SemaphoreType.DMA((sum(counts),)),
            ],
            compiler_params=pltpu.CompilerParams(collective_id=0, has_side_effects=True),
            name="relayed",
        )(right_side, coefficient)
        return (alpha * precond, right_side - alpha * image,
                precond - alpha * twice, image - alpha * image_twice)

    placed = (P(*AXES), P(*AXES))
    return jax.shard_map(
        shards, mesh=mesh, in_specs=placed, out_specs=(P(*AXES),) * 4, check_vma=False
    )
```
